32 devices in a mesh: rows: 4 (over y, x), cols: 8 (over z, core).
Axes of the slice: x: 2, y: 2, z: 4, core: 2. Of those that a mesh axis runs over, the one named last changes fastest.
Arguments:
- latent1: bfloat16 [64, 512, 320], P('rows', 'cols'), may hold values from -15 to 15, as said below
- norm1a_g: float32 [320], replicated, may hold values from 0.25 to 1.75
- norm1a_b: float32 [320], replicated, may hold values from -3 to 3
- conv1a_w: bfloat16 [3, 3, 320, 320], replicated, may hold values from -0.109375 to 0.109375
- norm1b_g: float32 [320], replicated, may hold values from 0.25 to 1.75
- norm1b_b: float32 [320], replicated, may hold values from -3 to 3
- conv1b_w: bfloat16 [3, 3, 320, 320], replicated, may hold values from -0.109375 to 0.109375
- conv1b_b: float32 [320], replicated, may hold values from -3 to 3
- feat3: bfloat16 [16, 128, 1280], P('rows', 'cols'), may hold values from -15 to 15, as said below
- adapter3: bfloat16 [16, 128, 1280], P('rows', 'cols'), may hold values from -15 to 15, as said below
- norm3a_g: float32 [1280], replicated, may hold values from 0.25 to 1.75
- norm3a_b: float32 [1280], replicated, may hold values from -3 to 3
- conv3a_w: bfloat16 [3, 3, 1280, 1280], P(None, None, None, 'cols'), may hold values from -0.0546875 to 0.0546875
- norm3b_g: float32 [1280], P('cols'), may hold values from 0.25 to 1.75
- norm3b_b: float32 [1280], P('cols'), may hold values from -3 to 3
- conv3b_w: bfloat16 [3, 3, 1280, 1280], P(None, None, None, 'cols'), may hold values from -0.0546875 to 0.0546875
- conv3b_b: float32 [1280], P('cols'), may hold values from -3 to 3
Outputs:
- out1: bfloat16 [64, 512, 320], P('rows', 'cols')
- out3: bfloat16 [16, 128, 1280], P('rows', None, 'cols')
The draws below stay inside these ranges and needn't reach their ends.
Inputs may be any that keep to these rules, and one draw needn't show every extreme that they name: `latent1`: real values. `feat3`: real values. `adapter3`: real values.
All inputs are finite; a program needn't handle non-finite values.
Results may differ from the reference program's by a relative error of at most 0.0052.
Values may be sent and summed in bfloat16 or wider, within the bound.
No kernel may reach another device: no remote copies, remote signals or barrier semaphores. Data moves between devices by JAX's collectives and lax.ppermute only.
A program may use at most 128 MiB of HBM per device.

```python
import jax
import jax.numpy as jnp
from jax import lax

C1 = 320
C3 = 1280
R1 = 64
K1 = 512
R3 = 16
W3 = 128


def spread_field(key, height, width, chans):
    key_noise, key_chan = jax.random.split(key, 2)
    row_pos = jnp.arange(height, dtype=jnp.float32) / max(height - 1, 1)
    col_pos = jnp.arange(width, dtype=jnp.float32) / max(width - 1, 1)
    chan_shift = jnp.clip(0.4 * jax.random.normal(key_chan, (chans,), jnp.float32), -1.0, 1.0)
    noise = jnp.clip(jax.random.normal(key_noise, (height, width, chans), jnp.float32), -4.0, 4.0)
    scale = 1.0 + 2.0 * row_pos
    offset = 1.5 * row_pos[:, None, None] - 0.5 * col_pos[None, :, None] + chan_shift[None, None, :]
    return noise * scale[:, None, None] + offset


def draw_latent1(key, part):
    return spread_field(jax.random.fold_in(key, 11), R1, K1, C1).astype(jnp.bfloat16)


def draw_feat3(key, part):
    return spread_field(jax.random.fold_in(key, 12), R3, W3, C3).astype(jnp.bfloat16)


def draw_adapter3(key, part):
    return spread_field(jax.random.fold_in(key, 13), R3, W3, C3).astype(jnp.bfloat16)


def level_of(stream_key, extent, shards, smallest, largest):
    level = 1.0
    for position, blocks in shards:
        draws = jax.random.uniform(jax.random.fold_in(jax.random.fold_in(stream_key, 6), position), (blocks,), jnp.float32, smallest / len(shards), largest / len(shards))
        level = level * jnp.repeat(jnp.exp(draws), extent[position] // blocks).reshape((-1,) + (1,) * (len(extent) - 1 - position))
    return level


def centred(stream_key, dims, scale, reach, shards=(), kind=jnp.bfloat16):
    level = level_of(stream_key, dims, shards, -0.22, 0.18) if shards else 1.0
    array = jax.random.normal(stream_key, dims, jnp.float32) * scale * level
    return jnp.minimum(jnp.maximum(array, -reach), reach).astype(kind)


def setup_inputs(seed: int = 0) -> dict:
    key_list = jax.random.split(jax.random.key(seed), 18)
    latent1 = draw_latent1(jax.random.fold_in(key_list[17], 71), 0)
    norm1a_g = jnp.clip(1.0 + 0.15 * jax.random.normal(key_list[1], (C1,), jnp.float32), 0.25, 1.75)
    norm1a_b = centred(key_list[2], (C1,), 0.5, 3.0, (), jnp.float32)
    conv1a_w = centred(key_list[3], (3, 3, C1, C1), (9 * C1) ** -0.5, 0.109375)
    norm1b_g = jnp.clip(1.0 + 0.15 * jax.random.normal(key_list[4], (C1,), jnp.float32), 0.25, 1.75)
    norm1b_b = centred(key_list[5], (C1,), 0.5, 3.0, (), jnp.float32)
    conv1b_w = centred(key_list[6], (3, 3, C1, C1), (9 * C1) ** -0.5, 0.109375)
    conv1b_b = centred(key_list[7], (C1,), 0.5, 3.0, (), jnp.float32)
    feat3 = draw_feat3(jax.random.fold_in(key_list[17], 71), 0)
    adapter3 = draw_adapter3(jax.random.fold_in(key_list[17], 71), 0)
    norm3a_g = jnp.clip(1.0 + 0.15 * jax.random.normal(key_list[10], (C3,), jnp.float32), 0.25, 1.75)
    norm3a_b = centred(key_list[11], (C3,), 0.5, 3.0, (), jnp.float32)
    conv3a_w = centred(key_list[12], (3, 3, C3, C3), (9 * C3) ** -0.5, 0.0546875, ((3, 8),))
    norm3b_g = jnp.clip(1.0 + 0.15 * jax.random.normal(key_list[13], (C3,), jnp.float32), 0.25, 1.75)
    norm3b_b = centred(key_list[14], (C3,), 0.5, 3.0, ((0, 8),), jnp.float32)
    conv3b_w = centred(key_list[15], (3, 3, C3, C3), (9 * C3) ** -0.5, 0.0546875, ((3, 8),))
    conv3b_b = centred(key_list[16], (C3,), 0.5, 3.0, ((0, 8),), jnp.float32)
    return {"latent1": latent1, "norm1a_g": norm1a_g, "norm1a_b": norm1a_b, "conv1a_w": conv1a_w, "norm1b_g": norm1b_g, "norm1b_b": norm1b_b, "conv1b_w": conv1b_w, "conv1b_b": conv1b_b, "feat3": feat3, "adapter3": adapter3, "norm3a_g": norm3a_g, "norm3a_b": norm3a_b, "conv3a_w": conv3a_w, "norm3b_g": norm3b_g, "norm3b_b": norm3b_b, "conv3b_w": conv3b_w, "conv3b_b": conv3b_b}


norm_groups = 32
norm_eps = 1e-05

def conv_same(field, kernel):
    return lax.conv_general_dilated(field[None], kernel, (1, 1), ((1, 1), (1, 1)), dimension_numbers=('NHWC', 'HWIO', 'NHWC'), preferred_element_type=jnp.float32)[0]

def group_silu(value, gain, shift):
    height, width, chans = value.shape
    grouped = value.astype(jnp.float32).reshape(height, width, norm_groups, chans // norm_groups)
    count = height * width * (chans // norm_groups)
    mean = lax.optimization_barrier(jnp.sum(grouped, axis=(0, 1, 3))) / count
    square = lax.optimization_barrier(jnp.sum(grouped * grouped, axis=(0, 1, 3))) / count
    inverse = lax.rsqrt(square - mean * mean + norm_eps)
    normed = ((grouped - mean[:, None]) * inverse[:, None]).reshape(height, width, chans)
    return jax.nn.silu(normed * gain + shift).astype(jnp.bfloat16)

def reference(latent1, norm1a_g, norm1a_b, conv1a_w, norm1b_g, norm1b_b, conv1b_w, conv1b_b, feat3, adapter3, norm3a_g, norm3a_b, conv3a_w, norm3b_g, norm3b_b, conv3b_w, conv3b_b):
    act1 = group_silu(latent1, norm1a_g, norm1a_b)
    hid1 = conv_same(act1, conv1a_w)
    act2 = group_silu(hid1, norm1b_g, norm1b_b)
    out1 = (latent1.astype(jnp.float32) + conv_same(act2, conv1b_w) + conv1b_b).astype(jnp.bfloat16)
    joined = (feat3.astype(jnp.float32) + adapter3.astype(jnp.float32)).astype(jnp.bfloat16)
    act3 = group_silu(joined, norm3a_g, norm3a_b)
    hid3 = conv_same(act3, conv3a_w)
    act4 = group_silu(hid3, norm3b_g, norm3b_b)
    out3 = (joined.astype(jnp.float32) + conv_same(act4, conv3b_w) + conv3b_b).astype(jnp.bfloat16)
    return (out1, out3)
```

```python
import jax
import jax.numpy as jnp
from jax import lax
from jax.sharding import PartitionSpec as P

C1 = 320
C3 = 1280


norm_eps = 1e-05


def extended(block, sides, width):
    for axis, dim in sides:
        count = lax.axis_size(axis)
        forward = [(i, i + 1) for i in range(count - 1)]
        backward = [(target, source) for source, target in forward]
        low = lax.ppermute(
            lax.slice_in_dim(block, block.shape[dim] - width, None, axis=dim), axis, forward
        )
        high = lax.ppermute(lax.slice_in_dim(block, 0, width, axis=dim), axis, backward)
        block = jnp.concatenate([low, block, high], axis=dim)
    return block


def conv_valid(padded, kernel):
    return lax.conv_general_dilated(
        padded[None],
        kernel,
        (1, 1),
        "VALID",
        dimension_numbers=("NHWC", "HWIO", "NHWC"),
        preferred_element_type=jnp.float32,
    )[0]


def moments(value, group_width):
    height, width, chans = value.shape
    grouped = value.astype(jnp.float32).reshape(height, width, chans // group_width, group_width)
    return (jnp.sum(grouped, axis=(0, 1, 3)), jnp.sum(grouped * grouped, axis=(0, 1, 3)))


def normalize(value, sums, squares, count, gain, shift):
    height, width, chans = value.shape
    groups = sums.shape[0]
    mean = sums / count
    inverse = lax.rsqrt(squares / count - mean * mean + norm_eps)
    grouped = value.astype(jnp.float32).reshape(height, width, groups, chans // groups)
    normed = ((grouped - mean[:, None]) * inverse[:, None]).reshape(height, width, chans)
    return jax.nn.silu(normed * gain + shift).astype(jnp.bfloat16)


def totals(vector):
    names = ("rows", "cols")
    count = lax.axis_size(names)
    copies = jnp.broadcast_to(vector, (count,) + vector.shape)
    return jnp.sum(lax.all_to_all(copies, names, 0, 0), axis=0)


def inside(height, width):
    row = lax.axis_index("rows") * height - 2 + jnp.arange(height + 4, dtype=jnp.int32)
    col = lax.axis_index("cols") * width - 2 + jnp.arange(width + 4, dtype=jnp.int32)
    row_ok = (row >= 0) & (row < height * lax.axis_size("rows"))
    col_ok = (col >= 0) & (col < width * lax.axis_size("cols"))
    return (row_ok[:, None] & col_ok[None, :])[:, :, None]


def folder(kernel, total, piece):
    height = total.shape[0]
    width = total.shape[1]
    count = piece.shape[2]
    wide = jnp.pad(piece, ((0, 0), (1, 1), (0, 0)))
    taps = [wide[dy : dy + height, dx : dx + width, :] for dy in range(3) for dx in range(3)]
    patches = jnp.concatenate(taps, axis=2).reshape(height * width, 9 * count)
    weights = kernel.reshape(9 * count, kernel.shape[3])
    product = jnp.dot(patches, weights, preferred_element_type=jnp.float32)
    return product.reshape(height, width, kernel.shape[3])


def body(
    latent1,
    norm1a_g,
    norm1a_b,
    conv1a_w,
    norm1b_g,
    norm1b_b,
    conv1b_w,
    conv1b_b,
    feat3,
    adapter3,
    norm3a_g,
    norm3a_b,
    conv3a_w,
    norm3b_g,
    norm3b_b,
    conv3b_w,
    conv3b_b,
):
    rows_one = latent1.shape[0]
    cols_one = latent1.shape[1]
    width_one = C1 // 32
    count_one = rows_one * cols_one * lax.axis_size("rows") * lax.axis_size("cols") * width_one
    joined = (feat3.astype(jnp.float32) + adapter3.astype(jnp.float32)).astype(jnp.bfloat16)
    shard = conv3a_w.shape[3]
    height = feat3.shape[0]
    width = feat3.shape[1] * lax.axis_size("cols")
    width_three = C3 // 32
    count_three = height * width * lax.axis_size("rows") * width_three
    zero = jnp.zeros((), jnp.bfloat16)
    raw = extended(latent1, (("rows", 0), ("cols", 1)), 2)
    edged_tile = extended(joined, (("rows", 0),), 1)
    whole = lax.all_gather(edged_tile, "cols", axis=1, tiled=True)
    first = totals(jnp.concatenate(moments(latent1, width_one) + moments(joined, width_three)))
    sums, squares, sums_three, squares_three = jnp.split(first, 4)
    ok = inside(rows_one, cols_one)
    act1 = jnp.where(ok, normalize(raw, sums, squares, count_one, norm1a_g, norm1a_b), zero)
    hid1 = conv_valid(act1, conv1a_w)
    local = lax.dynamic_slice_in_dim(whole[1:-1], lax.axis_index("cols") * shard, shard, 2)
    line_ids = lax.axis_index("rows") * height - 1 + jnp.arange(height + 2, dtype=jnp.int32)
    line_ok = (line_ids >= 0) & (line_ids < height * lax.axis_size("rows"))
    act_whole = normalize(whole, sums_three, squares_three, count_three, norm3a_g, norm3a_b)
    act_whole = jnp.where(line_ok[:, None, None], act_whole, zero)
    hid3 = conv_valid(jnp.pad(act_whole, ((0, 0), (1, 1), (0, 0))), conv3a_w)
    pieces = moments(hid3, width_three)
    spread = [
        jnp.where(
            jnp.arange(32) // part.shape[0] == lax.axis_index("cols"), jnp.tile(part, 32 // part.shape[0]), 0.0
        )
        for part in pieces
    ]
    second_sums = totals(jnp.concatenate(moments(hid1[1:-1, 1:-1], width_one) + tuple(spread)))
    sums_two, squares_two, sums_four, squares_four = jnp.split(second_sums, 4)
    own = shard // width_three
    start = lax.axis_index("cols") * own
    act4 = normalize(
        hid3,
        lax.dynamic_slice_in_dim(sums_four, start, own),
        lax.dynamic_slice_in_dim(squares_four, start, own),
        count_three,
        norm3b_g,
        norm3b_b,
    )
    edged_two = extended(act4, (("rows", 0),), 1)
    whole_two = lax.all_gather(edged_two, "cols", axis=2, tiled=True)
    act2 = normalize(hid1, sums_two, squares_two, count_one, norm1b_g, norm1b_b)
    act2 = jnp.where(ok[1:-1, 1:-1], act2, zero)
    out1 = (latent1.astype(jnp.float32) + conv_valid(act2, conv1b_w) + conv1b_b).astype(jnp.bfloat16)
    empty = jnp.zeros((height, width, shard), jnp.float32)
    second = folder(conv3b_w, empty, whole_two)
    out3 = (local.astype(jnp.float32) + second + conv3b_b).astype(jnp.bfloat16)
    return (out1, out3)


def solution(mesh):
    placed = (
        P("rows", "cols", None),
        P(),
        P(),
        P(),
        P(),
        P(),
        P(),
        P(),
        P("rows", "cols", None),
        P("rows", "cols", None),
        P(),
        P(),
        P(None, None, None, "cols"),
        P("cols"),
        P("cols"),
        P(None, None, None, "cols"),
        P("cols"),
    )
    return jax.shard_map(
        body,
        mesh=mesh,
        in_specs=placed,
        out_specs=(P("rows", "cols", None), P("rows", None, "cols")),
        check_vma=False,
    )
```

```python
import functools

import jax
import jax.numpy as jnp
from jax import lax
from jax.experimental import pallas as pl
from jax.experimental.pallas import tpu as pltpu
from jax.sharding import PartitionSpec as P


groups = 32
norm_eps = 1e-05
side = 16
bf16 = jnp.bfloat16
f32 = jnp.float32
both = ("rows", "cols")


def call(kernel, out_shape, args, scratch=(), flops=0, outside=(), grant=24):
    return pl.pallas_call(
        kernel,
        out_shape=out_shape,
        in_specs=[pl.BlockSpec(memory_space=pl.ANY if at in outside else pltpu.VMEM) for at in range(len(args))],
        out_specs=jax.tree.map(lambda _: pl.BlockSpec(memory_space=pltpu.VMEM), out_shape),
        scratch_shapes=list(scratch),
        compiler_params=pltpu.CompilerParams(vmem_limit_bytes=grant * 1024 * 1024),
        cost_estimate=pl.CostEstimate(flops=flops, bytes_accessed=0, transcendentals=0),
    )(*args)


def shape(dims, kind=f32):
    return jax.ShapeDtypeStruct(dims, kind)


def exact_dot(left, right):
    return lax.dot_general(
        left, right, (((1,), (0,)), ((), ())), precision=lax.Precision.HIGHEST, preferred_element_type=f32
    )


def to_groups(chans, width, first, lane):
    chan = lax.broadcasted_iota(jnp.int32, (chans, 128), 0) + first
    low = (lax.broadcasted_iota(jnp.int32, (chans, 128), 1) - lane) * width
    return jnp.where((chan >= low) & (chan < low + width), 1.0, 0.0).astype(f32)


def from_groups(chan, width, lane):
    low = (lax.broadcasted_iota(jnp.int32, (128, chan.shape[1]), 0) - lane) * width
    return jnp.where((chan >= low) & (chan < low + width), 1.0, 0.0).astype(f32)


def group_row(sums, squares, width, first, lane):
    chans = sums.shape[1]
    row = exact_dot(jnp.broadcast_to(sums, (8, chans)), to_groups(chans, width, first, lane))
    row += exact_dot(jnp.broadcast_to(squares, (8, chans)), to_groups(chans, width, first, lane + groups))
    return row[0:1]


def statistics(total, count, width, lane, chan):
    total = jnp.broadcast_to(total, (8, 128)) / count
    mean = exact_dot(total, from_groups(chan, width, lane))[0:1]
    square = exact_dot(total, from_groups(chan, width, lane + groups))[0:1]
    return mean, lax.rsqrt(square - mean * mean + norm_eps)


def lane_ids(chans):
    return lax.broadcasted_iota(jnp.int32, (1, chans), 1)


def activate(value, mean, scale, shift):
    half = ((value - mean) * scale + shift) * 0.5
    return half + half * jnp.tanh(half)


def input_sums_kernel(widths, latent_ref, joined_ref, gain_ref, shift_ref, out_ref):
    def sums_of(ref):
        def step(row, carry):
            value = ref[row].astype(f32)
            return (
                carry[0] + jnp.sum(value, axis=0, keepdims=True),
                carry[1] + jnp.sum(value * value, axis=0, keepdims=True),
            )

        start = jnp.zeros((1, ref.shape[2]), f32)
        return lax.fori_loop(0, ref.shape[0], step, (start, start))

    row = group_row(*sums_of(latent_ref), widths[0], 0, 0)
    row += group_row(*sums_of(joined_ref), widths[1], 0, 2 * groups)
    count = out_ref.shape[0]
    shard = gain_ref.shape[1]
    room = (out_ref.shape[2] - 128) // 2
    out_ref[...] = jnp.zeros_like(out_ref)
    out_ref[:, :, 0:128] = jnp.broadcast_to(row[None], (count, 1, 128))
    out_ref[:, :, pl.ds(128, shard)] = jnp.broadcast_to(gain_ref[...][None], (count, 1, shard))
    out_ref[:, :, pl.ds(128 + room, shard)] = jnp.broadcast_to(shift_ref[...][None], (count, 1, shard))


def pack_level_one(weight_ref, packed_ref):
    chans = weight_ref.shape[2]
    for dy in range(3):
        for dx in range(3):
            packed_ref[pl.ds(dy * chans, chans), pl.ds(dx * chans, chans)] = weight_ref[dy, dx]


def store_taps(act_ref, block, value, blocks=None):
    chans = value.shape[1]
    for tap in range(3):
        if blocks is None or 0 <= block - tap < blocks:
            act_ref[block - tap, :, pl.ds(tap * chans, chans)] = value


def products(act_ref, packed_ref, prod_ref):
    blocks, wide, depth = act_ref.shape
    left = act_ref[...].reshape(blocks * wide, depth)
    prod_ref[pl.ds(8, blocks * wide), :] = jnp.dot(left, packed_ref[...], preferred_element_type=f32)


def shifted_sum(prod_ref, block, wide, keep):
    chans = prod_ref.shape[1] // 3
    rows = prod_ref[pl.ds(pl.multiple_of(block * wide, 8), wide + 16), :]
    return (
        rows[7 : 7 + keep, 0:chans]
        + rows[8 : 8 + keep, chans : 2 * chans]
        + rows[9 : 9 + keep, 2 * chans : 3 * chans]
    )


def edge_flags(sizes):
    row, col = lax.axis_index("rows"), lax.axis_index("cols")
    return row > 0, row < sizes[0] - 1, col > 0, col < sizes[1] - 1


def level_one_first_kernel(
    count, width, sizes, latent_ref, top_ref, low_ref, side_ref, sums_ref, gain_ref, shift_ref, weight_ref,
    hid_ref, row_ref, act_ref, packed_ref, prod_ref,
):
    rows, cols, chans = latent_ref.shape
    wide = cols + side
    has_top, has_low, has_left, has_right = edge_flags(sizes)
    total = jnp.sum(sums_ref[:, :, 0:128], axis=0)
    mean, inverse = statistics(total, count, width, 0, lane_ids(chans))
    scale, shift = inverse * gain_ref[...], shift_ref[...]
    pack_level_one(weight_ref, packed_ref)
    place = lax.broadcasted_iota(jnp.int32, (side, chans), 0)
    blocks = rows + 3

    def fill(block, main, main_ok, right_ok, left_ok, limit=None):
        edge = activate(side_ref[block].astype(f32), mean, scale, shift)
        keep = ((place < side // 2) & right_ok) | ((place >= side // 2) & left_ok)
        edge = jnp.where(keep, edge, 0.0)
        value = activate(main.astype(f32), mean, scale, shift)
        value = jnp.where(main_ok, value, 0.0)
        store_taps(act_ref, block, jnp.concatenate([value, edge], axis=0).astype(bf16), limit)

    never = has_top & jnp.logical_not(has_top)
    fill(0, latent_ref[0], never, never, has_left & has_top, blocks)
    fill(1, top_ref[0], has_top, has_right & has_top, has_left & has_top, blocks)
    fill(2, top_ref[1], has_top, has_right & has_top, has_left, blocks)

    def main_row(line, carry):
        fill(line + 3, latent_ref[line], True, has_right, has_left & ((line < rows - 1) | has_low))
        return carry

    lax.fori_loop(0, rows, main_row, 0)
    fill(rows + 3, low_ref[0], has_low, has_right & has_low, has_left & has_low, blocks)
    fill(rows + 4, low_ref[1], has_low, has_right & has_low, never, blocks)

    products(act_ref, packed_ref, prod_ref)

    def combine(block, carry):
        value = shifted_sum(prod_ref, block, wide, wide)
        hid_ref[block] = value
        main = value[0:cols]
        inner = jnp.where((block >= 2) & (block < rows + 2), 1.0, 0.0)
        main = main * inner
        return (
            carry[0] + jnp.sum(main, axis=0, keepdims=True),
            carry[1] + jnp.sum(main * main, axis=0, keepdims=True),
        )

    start = jnp.zeros((1, chans), f32)
    sums, squares = lax.fori_loop(0, blocks, combine, (start, start))
    row_ref[...] = group_row(sums, squares, width, 0, 0)


def level_one_second_kernel(
    count, width, sizes, hid_ref, latent_ref, sums_ref, gain_ref, shift_ref, weight_ref, bias_ref,
    out_ref, act_ref, packed_ref, prod_ref,
):
    rows, cols, chans = latent_ref.shape
    wide = cols + side
    has_top, has_low, has_left, has_right = edge_flags(sizes)
    total = jnp.sum(sums_ref[...], axis=0)
    mean, inverse = statistics(total, count, width, 0, lane_ids(chans))
    scale, shift = inverse * gain_ref[...], shift_ref[...]
    pack_level_one(weight_ref, packed_ref)
    place = lax.broadcasted_iota(jnp.int32, (wide, chans), 0)
    blocks = rows + 1

    def fill(block, main_ok, right_ok, left_ok, limit=None):
        value = activate(hid_ref[block], mean, scale, shift)
        keep = ((place < cols) & main_ok) | ((place == cols) & right_ok) | ((place == wide - 1) & left_ok)
        store_taps(act_ref, block, jnp.where(keep, value, 0.0).astype(bf16), limit)

    never = has_top & jnp.logical_not(has_top)
    fill(0, never, never, has_left & has_top, blocks)
    fill(1, has_top, has_right & has_top, has_left, blocks)

    def main_row(line, carry):
        fill(line + 2, True, has_right, has_left & ((line < rows - 1) | has_low))
        return carry

    lax.fori_loop(0, rows - 1, main_row, 0)
    fill(rows + 1, True, has_right, has_left & has_low, blocks)
    fill(rows + 2, has_low, has_right & has_low, never, blocks)

    products(act_ref, packed_ref, prod_ref)

    def combine(line, carry):
        value = shifted_sum(prod_ref, line + 1, wide, cols)
        out_ref[line] = (latent_ref[line].astype(f32) + value + bias_ref[...]).astype(bf16)
        return carry

    lax.fori_loop(0, rows, combine, 0)


def level_three_taps(left, right):
    dims = (((1,), (right[1],)), ((), ()))
    return lax.dot_general(left.reshape(-1, left.shape[2]), right[0], dims, preferred_element_type=f32)


def level_three_sum(prod_ref, line, cols, shard):
    lanes = pl.ds(line * cols, cols)
    place = lax.broadcasted_iota(jnp.int32, (shard, cols), 1)
    left = pltpu.roll(prod_ref[pl.ds(0, shard), lanes], 1, 1)
    right = pltpu.roll(prod_ref[pl.ds(2 * shard, shard), lanes], cols - 1, 1)
    left = jnp.where(place == 0, 0.0, left)
    right = jnp.where(place == cols - 1, 0.0, right)
    return left + prod_ref[pl.ds(shard, shard), lanes] + right


def level_three_first_kernel(
    count, width, sizes, near_ref, far_ref, near_edges_ref, far_edges_ref, sums_ref, gain_ref, shift_ref, weight_hbm, other_ref,
    hid_ref, local_ref, row_ref, act_ref, raw_ref, prod_ref, weight_ref, weight_sem,
):
    chips, height, tile, chans = near_ref.shape
    shard, cols = hid_ref.shape[1:]
    lines = height + 2
    fetch = pltpu.make_async_copy(weight_hbm, weight_ref, weight_sem)
    fetch.start()
    col_id = lax.axis_index("cols")
    has_top, has_low, _, _ = edge_flags(sizes)
    total = jnp.sum(sums_ref[:, :, 0:128], axis=0)
    mean, inverse = statistics(total, count, width, 2 * groups, lane_ids(chans))
    scale, shift = inverse * gain_ref[...], shift_ref[...]
    for hop in range(chips):
        for flip, (ref, edges) in enumerate(((near_ref, near_edges_ref), (far_ref, far_edges_ref))):
            place = pl.ds(pl.multiple_of((col_id ^ (2 * hop + flip)) * tile, tile), tile)

            def fill(line, carry):
                raw = ref[hop, line]
                raw_ref[line, place, :] = raw
                act_ref[line + 1, place, :] = activate(raw.astype(f32), mean, scale, shift).astype(bf16)
                return carry

            lax.fori_loop(0, height, fill, 0)
            for at, line, keep in ((0, 0, has_top), (1, lines - 1, has_low)):
                value = activate(edges[hop, at].astype(f32), mean, scale, shift)
                act_ref[line, place, :] = jnp.where(keep, value, 0.0).astype(bf16)

    chan = lax.broadcasted_iota(jnp.int32, (shard, chans), 1)
    wanted = lax.broadcasted_iota(jnp.int32, (shard, chans), 0) + col_id * shard
    pick = jnp.where(chan == wanted, 1.0, 0.0).astype(bf16)
    raw = raw_ref[...].reshape(height * cols, chans)
    local = level_three_taps(pick[None], (raw, 1)).astype(bf16)
    for line in range(height):
        local_ref[line] = local[:, line * cols : (line + 1) * cols]
    fetch.wait()
    total = None
    for dy in range(3):
        right = act_ref[pl.ds(dy, height)].reshape(height * cols, chans)
        part = level_three_taps(weight_ref[dy], (right, 1))
        total = part if total is None else total + part
    prod_ref[...] = total

    sums = squares = jnp.zeros((shard, cols), f32)
    for line in range(height):
        value = level_three_sum(prod_ref, line, cols, shard)
        hid_ref[line] = value.astype(bf16)
        sums, squares = sums + value, squares + value * value
    row = other_ref[...]
    for part, lane in ((sums, 2 * groups), (squares, 3 * groups)):
        column = jnp.sum(part, axis=1, keepdims=True)
        row += jnp.sum(column * to_groups(shard, width, col_id * shard, lane), axis=0, keepdims=True)
    row_ref[...] = jnp.broadcast_to(row[None], row_ref.shape)


def level_three_second_kernel(
    count, width, sizes, near_ref, far_ref, near_edges_ref, far_edges_ref, local_ref, sums_ref, affine_ref, weight_hbm, bias_ref,
    out_ref, act_ref, prod_ref, weight_ref, weight_sem,
):
    chips, height, shard, cols = near_ref.shape
    lines = height + 2
    fetch = pltpu.make_async_copy(weight_hbm, weight_ref, weight_sem)
    fetch.start()
    room = (affine_ref.shape[2] - 128) // 2
    row_id, col_id = lax.axis_index("rows"), lax.axis_index("cols")
    has_top, has_low, _, _ = edge_flags(sizes)
    total = jnp.sum(sums_ref[...], axis=0) / count
    first = row_id * sizes[1]
    place = lax.broadcasted_iota(jnp.int32, (shard, 128), 0)
    lane_at = lax.broadcasted_iota(jnp.int32, (shard, 128), 1)

    def column_of(row):
        found = jnp.zeros((shard, 128), f32)
        for start in range(0, room, 128):
            found += jnp.where(lane_at + start == place, row[:, start : start + 128], 0.0)
        return jnp.sum(found, axis=1, keepdims=True)

    for hop in range(chips):
        for flip, (ref, edges) in enumerate(((near_ref, near_edges_ref), (far_ref, far_edges_ref))):
            source = col_id ^ (2 * hop + flip)
            row = affine_ref[first + source]
            mean = jnp.sum(to_groups(shard, width, source * shard, 2 * groups) * total, axis=1, keepdims=True)
            square = jnp.sum(to_groups(shard, width, source * shard, 3 * groups) * total, axis=1, keepdims=True)
            scale = lax.rsqrt(square - mean * mean + norm_eps) * column_of(row[:, 128 : 128 + room])
            shift = column_of(row[:, 128 + room : 128 + 2 * room])
            chan = pl.ds(pl.multiple_of(source * shard, 16), shard)
            for line in range(lines):
                raw = edges[hop, min(line, 1)] if line in (0, lines - 1) else ref[hop, line - 1]
                value = activate(raw.astype(f32), mean, scale, shift)
                if line == 0:
                    value = jnp.where(has_top, value, 0.0)
                if line == lines - 1:
                    value = jnp.where(has_low, value, 0.0)
                act_ref[chan, pl.ds(line * cols, cols)] = value.astype(bf16)

    fetch.wait()
    total = None
    for dy in range(3):
        right = act_ref[:, pl.ds(dy * cols, height * cols)]
        part = level_three_taps(weight_ref[dy], (right, 0))
        total = part if total is None else total + part
    prod_ref[...] = total
    bias = column_of(bias_ref[...])
    for line in range(height):
        value = level_three_sum(prod_ref, line, cols, shard)
        out_ref[line] = (local_ref[line].astype(f32) + value + bias).astype(bf16)


def neighbours(low_edge, high_edge, axis):
    count = lax.axis_size(axis)
    forward = [(i, i + 1) for i in range(count - 1)]
    backward = [(target, source) for source, target in forward]
    return lax.ppermute(high_edge, axis, forward), lax.ppermute(low_edge, axis, backward)


def hop_to(value, step):
    return lax.ppermute(value, "cols", [(i, i ^ step) for i in range(lax.axis_size("cols"))])


def exchange(sent):
    return lax.all_to_all(sent, both, 0, 0)


def gathered(own, received, sums):
    *received, sums = lax.optimization_barrier((*received, sums))
    near = jnp.stack([own] + received)
    top, low = neighbours(near[:, 0:1], near[:, -1:], "rows")
    edges = jnp.concatenate([top, low], axis=1)
    return near, hop_to(near, 1), edges, hop_to(edges, 1), sums


def body(
    latent1, norm1a_g, norm1a_b, conv1a_w, norm1b_g, norm1b_b, conv1b_w, conv1b_b, feat3, adapter3,
    norm3a_g, norm3a_b, conv3a_w, norm3b_g, norm3b_b, conv3b_w, conv3b_b,
):
    sizes = (lax.axis_size("rows"), lax.axis_size("cols"))
    devices = sizes[0] * sizes[1]
    chips = sizes[1] // 2
    rows, cols, chans = latent1.shape
    wide = cols + side
    height, tile, deep = feat3.shape
    whole_cols = tile * sizes[1]
    shard = conv3a_w.shape[3]
    widths = (chans // groups, deep // groups)
    count_one = float(rows * cols * devices * widths[0])
    count_three = float(height * tile * devices * widths[1])
    row_of = lambda vector: vector.reshape(1, -1)

    top, low = neighbours(latent1[:2], latent1[-2:], "rows")
    joined = (feat3.astype(f32) + adapter3.astype(f32)).astype(bf16)
    edge = lambda at: jnp.concatenate([top[:, at], latent1[:, at], low[:, at]], axis=0)
    left, right = neighbours(edge(slice(0, 2)), edge(slice(cols - 2, cols)), "cols")
    beside = jnp.pad(right, ((1, 0), (0, side - 2), (0, 0))) + jnp.pad(left, ((0, 1), (side - 2, 0), (0, 0)))
    received = [hop_to(joined, 2 * k) for k in range(1, chips)]

    room = -(-shard // 128) * 128
    sent = call(
        functools.partial(input_sums_kernel, widths),
        shape((devices, 1, 128 + 2 * room)),
        (latent1, joined, row_of(norm3b_g), row_of(norm3b_b)),
    )
    sums = exchange(sent)
    near, far, near_edges, far_edges, sums = gathered(joined, received, sums)

    hid1, row_one = call(
        functools.partial(level_one_first_kernel, count_one, widths[0], sizes),
        (shape((rows + 3, wide, chans)), shape((1, 128))),
        (latent1, top, low, beside, sums, row_of(norm1a_g), row_of(norm1a_b), conv1a_w),
        (
            pltpu.VMEM((rows + 3, wide, 3 * chans), bf16),
            pltpu.VMEM((3 * chans, 3 * chans), bf16),
            pltpu.VMEM(((rows + 3) * wide + 16, 3 * chans), f32),
        ),
        flops=2 * rows * cols * 9 * chans * chans,
    )

    flops_three = 2 * height * whole_cols * 9 * deep * shard
    by_input = lambda weight: jnp.swapaxes(weight, 2, 3)
    tile_out = shape((height, shard, whole_cols), bf16)
    three_scratch = (
        pltpu.VMEM((3 * shard, height * whole_cols), f32),
        pltpu.VMEM((3, 3, shard, deep), bf16),
        pltpu.SemaphoreType.DMA,
    )
    hid3, local, sent_two = call(
        functools.partial(level_three_first_kernel, count_three, widths[1], sizes),
        (tile_out, tile_out, shape((devices, 1, 128))),
        (near, far, near_edges, far_edges, sums, row_of(norm3a_g), row_of(norm3a_b), by_input(conv3a_w), row_one),
        (pltpu.VMEM((height + 2, whole_cols, deep), bf16), pltpu.VMEM((height, whole_cols, deep), bf16)) + three_scratch,
        flops=flops_three,
        outside=(7,),
    )
    received = [hop_to(hid3, 2 * k) for k in range(1, chips)]
    sums_two = exchange(sent_two)
    near_two, far_two, near_edges_two, far_edges_two, sums_two = gathered(hid3, received, sums_two)

    out1 = call(
        functools.partial(level_one_second_kernel, count_one, widths[0], sizes),
        shape(latent1.shape, bf16),
        (hid1, latent1, sums_two, row_of(norm1b_g), row_of(norm1b_b), conv1b_w, row_of(conv1b_b)),
        (
            pltpu.VMEM((rows + 1, wide, 3 * chans), bf16),
            pltpu.VMEM((3 * chans, 3 * chans), bf16),
            pltpu.VMEM(((rows + 1) * wide + 16, 3 * chans), f32),
        ),
        flops=2 * rows * cols * 9 * chans * chans,
    )
    bias = jnp.pad(row_of(conv3b_b), ((0, 0), (0, room - shard)))
    out3 = call(
        functools.partial(level_three_second_kernel, count_three, widths[1], sizes),
        tile_out,
        (near_two, far_two, near_edges_two, far_edges_two, local, sums_two, sums, by_input(conv3b_w), bias),
        (pltpu.VMEM((deep, (height + 2) * whole_cols), bf16),) + three_scratch,
        flops=flops_three,
        outside=(7,),
    )
    return (out1, jnp.swapaxes(out3, 1, 2))


def solution(mesh):
    placed = (
        P("rows", "cols", None),
        P(),
        P(),
        P(),
        P(),
        P(),
        P(),
        P(),
        P("rows", "cols", None),
        P("rows", "cols", None),
        P(),
        P(),
        P(None, None, None, "cols"),
        P("cols"),
        P("cols"),
        P(None, None, None, "cols"),
        P("cols"),
    )
    return jax.shard_map(
        body,
        mesh=mesh,
        in_specs=placed,
        out_specs=(P("rows", "cols", None), P("rows", None, "cols")),
        check_vma=False,
    )
```

```python
import functools

import jax
import jax.numpy as jnp
from jax import lax
from jax.experimental import pallas as pl
from jax.experimental.pallas import tpu as pltpu
from jax.sharding import PartitionSpec as P


groups = 32
norm_eps = 1e-05
side = 16
bf16 = jnp.bfloat16
f32 = jnp.float32
both = ("rows", "cols")


def call(kernel, out_shape, args, scratch=(), flops=0, outside=(), outside_out=(), grant=24):
    made = pl.pallas_call(
        kernel,
        out_shape=out_shape,
        in_specs=[pl.BlockSpec(memory_space=pltpu.HBM if at in outside else pltpu.VMEM) for at in range(len(args))],
        out_specs=tuple(
            pl.BlockSpec(memory_space=pltpu.HBM if at in outside_out else pltpu.VMEM) for at in range(len(out_shape))
        ),
        scratch_shapes=list(scratch),
        compiler_params=pltpu.CompilerParams(vmem_limit_bytes=grant * 1024 * 1024),
        cost_estimate=pl.CostEstimate(flops=flops, bytes_accessed=0, transcendentals=0),
    )
    outs = made(*args)
    return outs if len(outs) > 1 else outs[0]


def shape(dims, kind=f32):
    return jax.ShapeDtypeStruct(dims, kind)


def pieces(value):
    high = value.astype(bf16)
    rest = value - high.astype(f32)
    middle = rest.astype(bf16)
    return high, middle, (rest - middle.astype(f32)).astype(bf16)


def joined_rows(first, second):
    place = lax.broadcasted_iota(jnp.int32, (16, first.shape[1]), 0)
    found = jnp.zeros((16, first.shape[1]), f32)
    for at, piece in enumerate(pieces(first) + pieces(second)):
        found = jnp.where(place == at, piece.astype(f32), found)
    return found.astype(bf16)


def ones_in_group(chan, low, width):
    return jnp.where((chan >= low) & (chan < low + width), 1.0, 0.0).astype(f32)


def to_groups(chans, width, first, lane):
    chan = lax.broadcasted_iota(jnp.int32, (chans, 128), 0) + first
    low = (lax.broadcasted_iota(jnp.int32, (chans, 128), 1) - lane) * width
    return ones_in_group(chan, low, width)


def from_groups(chan, width, lane):
    low = (lax.broadcasted_iota(jnp.int32, (128, chan.shape[1]), 0) - lane) * width
    return ones_in_group(chan, low, width)


def group_row(sums, squares, width, first, lane):
    sums = jnp.sum(sums, axis=0, keepdims=True)
    squares = jnp.sum(squares, axis=0, keepdims=True)
    member = to_groups(sums.shape[1], width, first, lane).astype(bf16)
    found = jnp.dot(joined_rows(sums, squares), member, preferred_element_type=f32)
    total = found[0:1] + found[1:2] + found[2:3]
    square = found[3:4] + found[4:5] + found[5:6]
    return total + pltpu.roll(jnp.broadcast_to(square, (8, 128)), groups, 1)[0:1]


def statistics(total, count, width, lane, chan):
    total = total / count
    moved = pltpu.roll(jnp.broadcast_to(total, (8, 128)), 128 - groups, 1)[0:1]
    member = from_groups(chan, width, lane).astype(bf16)
    found = jnp.dot(joined_rows(total, moved), member, preferred_element_type=f32)
    mean = found[0:1] + found[1:2] + found[2:3]
    square = found[3:4] + found[4:5] + found[5:6]
    return mean, lax.rsqrt(square - mean * mean + norm_eps)


def lane_ids(chans):
    return lax.broadcasted_iota(jnp.int32, (1, chans), 1)


def activate(value, mean, scale, shift):
    half = ((value - mean) * scale + shift) * 0.5
    return half + half * jnp.tanh(half)


def start_all(copies):
    made = [pltpu.make_async_copy(*copy) for copy in copies]
    for copy in made:
        copy.start()
    return made


def input_sums_kernel(
    widths, joined_ref, latent_hbm, gain_hbm, shift_hbm, out_ref, latent_ref, gain_ref, shift_ref, sems
):
    half = latent_ref.shape[0] // 2
    first, second = pl.ds(0, half), pl.ds(half, half)
    copies = start_all(
        (
            (latent_hbm.at[first], latent_ref.at[first], sems.at[0]),
            (latent_hbm.at[second], latent_ref.at[second], sems.at[1]),
            (gain_hbm, gain_ref, sems.at[2]),
            (shift_hbm, shift_ref, sems.at[3]),
        )
    )

    def sums_of(ref, begin, end, carry):
        def step(row, carry):
            value = ref[row].astype(f32)
            return carry[0] + folded(value), carry[1] + folded(value * value)

        return lax.fori_loop(begin, end, step, carry, unroll=True)

    def start(ref):
        zero = jnp.zeros((8, ref.shape[2]), f32)
        return zero, zero

    three = sums_of(joined_ref, 0, joined_ref.shape[0], start(joined_ref))
    row = group_row(*three, widths[1], 0, 2 * groups)
    copies[0].wait()
    one = sums_of(latent_ref, 0, half, start(latent_ref))
    copies[1].wait()
    one = sums_of(latent_ref, half, 2 * half, one)
    row += group_row(*one, widths[0], 0, 0)
    count = out_ref.shape[0]
    shard = gain_ref.shape[1]
    room = (out_ref.shape[2] - 128) // 2
    out_ref[...] = jnp.zeros_like(out_ref)
    out_ref[:, :, 0:128] = jnp.broadcast_to(row[None], (count, 1, 128))
    copies[2].wait()
    copies[3].wait()
    out_ref[:, :, pl.ds(128, shard)] = jnp.broadcast_to(gain_ref[...][None], (count, 1, shard))
    out_ref[:, :, pl.ds(128 + room, shard)] = jnp.broadcast_to(shift_ref[...][None], (count, 1, shard))


def pack_level_one(weight_ref, packed_ref):
    chans = weight_ref.shape[2]
    for dy in range(3):
        for dx in range(3):
            packed_ref[pl.ds(dy * chans, chans), pl.ds(dx * chans, chans)] = weight_ref[dy, dx]


def store_taps(act_ref, block, value, blocks=None):
    chans = value.shape[1]
    for tap in range(3):
        if blocks is None or 0 <= block - tap < blocks:
            act_ref[block - tap, :, pl.ds(tap * chans, chans)] = value


def products(act_ref, packed_ref, prod_ref):
    blocks, wide, depth = act_ref.shape
    left = act_ref[...].reshape(blocks * wide, depth)
    prod_ref[pl.ds(8, blocks * wide), :] = jnp.dot(left, packed_ref[...], preferred_element_type=f32)


def shifted_sum(prod_ref, start, keep):
    chans = prod_ref.shape[1] // 3
    rows = prod_ref[pl.ds(pl.multiple_of(start, 8), keep + 16), :]
    return (
        rows[7 : 7 + keep, 0:chans]
        + rows[8 : 8 + keep, chans : 2 * chans]
        + rows[9 : 9 + keep, 2 * chans : 3 * chans]
    )


def folded(value):
    return jnp.sum(value.reshape(value.shape[0] // 8, 8, value.shape[1]), axis=0)


def edge_flags(sizes):
    row, col = lax.axis_index("rows"), lax.axis_index("cols")
    return row > 0, row < sizes[0] - 1, col > 0, col < sizes[1] - 1


def level_one_first_kernel(
    count, width, sizes, latent_ref, top_ref, low_ref, side_ref, sums_ref, gain_ref, shift_ref, other_ref, weight_ref,
    hid_hbm, row_ref, act_ref, packed_ref, prod_ref, hid_ref, hid_sems,
):
    rows, cols, chans = latent_ref.shape
    wide = cols + side
    has_top, has_low, has_left, has_right = edge_flags(sizes)
    total = jnp.sum(sums_ref[:, :, 0:128], axis=0)
    mean, inverse = statistics(total, count, width, 0, lane_ids(chans))
    scale, shift = inverse * gain_ref[...], shift_ref[...]
    place = lax.broadcasted_iota(jnp.int32, (side, chans), 0)
    blocks = rows + 3

    def fill(block, main, main_ok, right_ok, left_ok, limit=None):
        edge = activate(side_ref[block].astype(f32), mean, scale, shift)
        keep = ((place < side // 2) & right_ok) | ((place >= side // 2) & left_ok)
        edge = jnp.where(keep, edge, 0.0)
        value = activate(main.astype(f32), mean, scale, shift)
        value = jnp.where(main_ok, value, 0.0)
        store_taps(act_ref, block, jnp.concatenate([value, edge], axis=0).astype(bf16), limit)

    never = has_top & jnp.logical_not(has_top)
    fill(0, latent_ref[0], never, never, has_left & has_top, blocks)
    fill(1, top_ref[0], has_top, has_right & has_top, has_left & has_top, blocks)
    fill(2, top_ref[1], has_top, has_right & has_top, has_left, blocks)

    def main_row(line, carry):
        fill(line + 3, latent_ref[line], True, has_right, has_left & ((line < rows - 1) | has_low))
        return carry

    lax.fori_loop(0, rows, main_row, 0, unroll=True)
    fill(rows + 3, low_ref[0], has_low, has_right & has_low, has_left & has_low, blocks)
    fill(rows + 4, low_ref[1], has_low, has_right & has_low, never, blocks)

    pack_level_one(weight_ref, packed_ref)
    products(act_ref, packed_ref, prod_ref)

    def combine(block, carry):
        inner = jnp.where((block >= 2) & (block < rows + 2), 1.0, 0.0)
        sums, squares = carry
        for at in range(0, wide, side):
            value = shifted_sum(prod_ref, block * wide + at, side)
            hid_ref[block, pl.ds(at, side), :] = value.astype(bf16)
            if at < cols:
                value = value * inner
                sums, squares = sums + folded(value), squares + folded(value * value)
        return sums, squares

    start = jnp.zeros((8, chans), f32)
    carry = (start, start)
    half = blocks // 2
    copies = []
    for at, (begin, end) in enumerate(((0, half), (half, blocks))):
        carry = lax.fori_loop(begin, end, combine, carry, unroll=True)
        part = pl.ds(begin, end - begin)
        copies += start_all(((hid_ref.at[part], hid_hbm.at[part], hid_sems.at[at]),))
    sums, squares = carry
    row = other_ref[...] + group_row(sums, squares, width, 0, 0)
    row_ref[...] = jnp.broadcast_to(row[None], row_ref.shape)
    for copy in copies:
        copy.wait()


def level_one_second_kernel(
    count, width, sizes, hid_ref, latent_ref, sums_ref, gain_ref, shift_ref, bias_ref, weight_ref,
    out_ref, act_ref, packed_ref, prod_ref,
):
    half = hid_ref.shape[0] // 2
    rows, cols, chans = latent_ref.shape
    wide = cols + side
    has_top, has_low, has_left, has_right = edge_flags(sizes)
    total = jnp.sum(sums_ref[...], axis=0)
    mean, inverse = statistics(total, count, width, 0, lane_ids(chans))
    scale, shift = inverse * gain_ref[...], shift_ref[...]
    place = lax.broadcasted_iota(jnp.int32, (wide, chans), 0)
    blocks = rows + 1

    def fill(block, main_ok, right_ok, left_ok, limit=None):
        value = activate(hid_ref[block].astype(f32), mean, scale, shift)
        keep = ((place < cols) & main_ok) | ((place == cols) & right_ok) | ((place == wide - 1) & left_ok)
        store_taps(act_ref, block, jnp.where(keep, value, 0.0).astype(bf16), limit)

    never = has_top & jnp.logical_not(has_top)
    fill(0, never, never, has_left & has_top, blocks)
    fill(1, has_top, has_right & has_top, has_left, blocks)

    def main_row(line, carry):
        fill(line + 2, True, has_right, has_left & ((line < rows - 1) | has_low))
        return carry

    lax.fori_loop(0, half - 2, main_row, 0, unroll=True)
    lax.fori_loop(half - 2, rows - 1, main_row, 0, unroll=True)
    fill(rows + 1, True, has_right, has_left & has_low, blocks)
    fill(rows + 2, has_low, has_right & has_low, never, blocks)

    pack_level_one(weight_ref, packed_ref)
    products(act_ref, packed_ref, prod_ref)


    def combine(line, carry):
        for at in range(0, cols, side):
            value = shifted_sum(prod_ref, (line + 1) * wide + at, side)
            cells = pl.ds(at, side)
            out_ref[line, cells, :] = (latent_ref[line, cells, :].astype(f32) + value + bias_ref[...]).astype(bf16)
        return carry

    lax.fori_loop(0, rows, combine, 0, unroll=True)


def level_three_taps(left, right):
    dims = (((1,), (right[1],)), ((), ()))
    return lax.dot_general(left.reshape(-1, left.shape[2]), right[0], dims, preferred_element_type=f32)


def level_three_sum(prod_ref, line, cols, shard):
    lanes = pl.ds(line * cols, cols)
    place = lax.broadcasted_iota(jnp.int32, (shard, cols), 1)
    left = pltpu.roll(prod_ref[pl.ds(0, shard), lanes], 1, 1)
    right = pltpu.roll(prod_ref[pl.ds(2 * shard, shard), lanes], cols - 1, 1)
    left = jnp.where(place == 0, 0.0, left)
    right = jnp.where(place == cols - 1, 0.0, right)
    return left + prod_ref[pl.ds(shard, shard), lanes] + right


def level_three_first_kernel(
    count, width, sizes, near_ref, far_ref, near_edges_ref, far_edges_ref, sums_ref, gain_ref, shift_ref, weight_hbm,
    hid_ref, local_ref, row_ref, act_ref, raw_ref, prod_ref, weight_ref, weight_sem,
):
    chips, height, tile, chans = near_ref.shape
    shard, cols = hid_ref.shape[1:]
    lines = height + 2
    fetch = pltpu.make_async_copy(weight_hbm, weight_ref, weight_sem)
    fetch.start()
    col_id = lax.axis_index("cols")
    has_top, has_low, _, _ = edge_flags(sizes)
    total = jnp.sum(sums_ref[:, :, 0:128], axis=0)
    mean, inverse = statistics(total, count, width, 2 * groups, lane_ids(chans))
    scale, shift = inverse * gain_ref[...], shift_ref[...]
    for hop in range(chips):
        for flip, (ref, edges) in enumerate(((near_ref, near_edges_ref), (far_ref, far_edges_ref))):
            place = pl.ds(pl.multiple_of((col_id ^ (2 * hop + flip)) * tile, tile), tile)

            def fill(line, carry):
                raw = ref[hop, line]
                raw_ref[line, place, :] = raw
                act_ref[line + 1, place, :] = activate(raw.astype(f32), mean, scale, shift).astype(bf16)
                return carry

            lax.fori_loop(0, height, fill, 0, unroll=True)
            for at, line, keep in ((0, 0, has_top), (1, lines - 1, has_low)):
                value = activate(edges[hop, at].astype(f32), mean, scale, shift)
                act_ref[line, place, :] = jnp.where(keep, value, 0.0).astype(bf16)

    chan = lax.broadcasted_iota(jnp.int32, (shard, chans), 1)
    wanted = lax.broadcasted_iota(jnp.int32, (shard, chans), 0) + col_id * shard
    pick = jnp.where(chan == wanted, 1.0, 0.0).astype(bf16)
    raw = raw_ref[...].reshape(height * cols, chans)
    local = level_three_taps(pick[None], (raw, 1)).astype(bf16)
    for line in range(height):
        local_ref[line] = local[:, line * cols : (line + 1) * cols]
    fetch.wait()
    total = None
    for dy in range(3):
        right = act_ref[pl.ds(dy, height)].reshape(height * cols, chans)
        part = level_three_taps(weight_ref[dy], (right, 1))
        total = part if total is None else total + part
    prod_ref[...] = total

    sums = squares = jnp.zeros((shard, cols), f32)
    for line in range(height):
        value = level_three_sum(prod_ref, line, cols, shard)
        hid_ref[line] = value.astype(bf16)
        sums, squares = sums + value, squares + value * value
    row = jnp.zeros((1, 128), f32)
    for part, lane in ((sums, 2 * groups), (squares, 3 * groups)):
        column = jnp.sum(part, axis=1, keepdims=True)
        row += jnp.sum(column * to_groups(shard, width, col_id * shard, lane), axis=0, keepdims=True)
    row_ref[...] = row


def level_three_second_kernel(
    count, width, sizes, near_ref, far_ref, near_edges_ref, far_edges_ref, local_ref, sums_ref, affine_ref, weight_hbm, bias_ref,
    out_ref, act_ref, prod_ref, weight_ref, weight_sem,
):
    chips, height, shard, cols = near_ref.shape
    lines = height + 2
    fetch = pltpu.make_async_copy(weight_hbm, weight_ref, weight_sem)
    fetch.start()
    room = (affine_ref.shape[2] - 128) // 2
    row_id, col_id = lax.axis_index("rows"), lax.axis_index("cols")
    has_top, has_low, _, _ = edge_flags(sizes)
    total = jnp.sum(sums_ref[...], axis=0) / count
    first = row_id * sizes[1]
    place = lax.broadcasted_iota(jnp.int32, (shard, 128), 0)
    lane_at = lax.broadcasted_iota(jnp.int32, (shard, 128), 1)

    def column_of(row):
        found = jnp.zeros((shard, 128), f32)
        for start in range(0, room, 128):
            found += jnp.where(lane_at + start == place, row[:, start : start + 128], 0.0)
        return jnp.sum(found, axis=1, keepdims=True)

    for hop in range(chips):
        for flip, (ref, edges) in enumerate(((near_ref, near_edges_ref), (far_ref, far_edges_ref))):
            source = col_id ^ (2 * hop + flip)
            row = affine_ref[first + source]
            mean = jnp.sum(to_groups(shard, width, source * shard, 2 * groups) * total, axis=1, keepdims=True)
            square = jnp.sum(to_groups(shard, width, source * shard, 3 * groups) * total, axis=1, keepdims=True)
            scale = lax.rsqrt(square - mean * mean + norm_eps) * column_of(row[:, 128 : 128 + room])
            shift = column_of(row[:, 128 + room : 128 + 2 * room])
            chan = pl.ds(pl.multiple_of(source * shard, 16), shard)
            for line in range(lines):
                raw = edges[hop, min(line, 1)] if line in (0, lines - 1) else ref[hop, line - 1]
                value = activate(raw.astype(f32), mean, scale, shift)
                if line == 0:
                    value = jnp.where(has_top, value, 0.0)
                if line == lines - 1:
                    value = jnp.where(has_low, value, 0.0)
                act_ref[chan, pl.ds(line * cols, cols)] = value.astype(bf16)

    fetch.wait()
    total = None
    for dy in range(3):
        right = act_ref[:, pl.ds(dy * cols, height * cols)]
        part = level_three_taps(weight_ref[dy], (right, 0))
        total = part if total is None else total + part
    prod_ref[...] = total
    bias = column_of(bias_ref[...])
    for line in range(height):
        value = level_three_sum(prod_ref, line, cols, shard)
        out_ref[line] = (local_ref[line].astype(f32) + value + bias).astype(bf16)


def neighbours(low_edge, high_edge, axis):
    count = lax.axis_size(axis)
    forward = [(i, i + 1) for i in range(count - 1)]
    backward = [(target, source) for source, target in forward]
    return lax.ppermute(high_edge, axis, forward), lax.ppermute(low_edge, axis, backward)


def hop_to(value, step):
    return lax.ppermute(value, "cols", [(i, i ^ step) for i in range(lax.axis_size("cols"))])


def exchange(sent):
    return lax.all_to_all(sent, both, 0, 0)


def gathered(own, received):
    near = jnp.stack([own] + received)
    top, low = neighbours(near[:, 0:1], near[:, -1:], "rows")
    edges = jnp.concatenate([top, low], axis=1)
    return near, hop_to(near, 1), edges, hop_to(edges, 1)


def body(
    latent1, norm1a_g, norm1a_b, conv1a_w, norm1b_g, norm1b_b, conv1b_w, conv1b_b, feat3, adapter3,
    norm3a_g, norm3a_b, conv3a_w, norm3b_g, norm3b_b, conv3b_w, conv3b_b,
):
    sizes = (lax.axis_size("rows"), lax.axis_size("cols"))
    devices = sizes[0] * sizes[1]
    chips = sizes[1] // 2
    rows, cols, chans = latent1.shape
    wide = cols + side
    height, tile, deep = feat3.shape
    whole_cols = tile * sizes[1]
    shard = conv3a_w.shape[3]
    widths = (chans // groups, deep // groups)
    count_one = float(rows * cols * devices * widths[0])
    count_three = float(height * tile * devices * widths[1])
    row_of = lambda vector: vector.reshape(1, -1)

    top, low = neighbours(latent1[:2], latent1[-2:], "rows")
    joined = (feat3.astype(f32) + adapter3.astype(f32)).astype(bf16)
    edge = lambda at: jnp.concatenate([top[:, at], latent1[:, at], low[:, at]], axis=0)
    left, right = neighbours(edge(slice(0, 2)), edge(slice(cols - 2, cols)), "cols")
    beside = jnp.pad(right, ((1, 0), (0, side - 2), (0, 0))) + jnp.pad(left, ((0, 1), (side - 2, 0), (0, 0)))
    received = [hop_to(joined, 2 * k) for k in range(1, chips)]

    room = -(-shard // 128) * 128
    sent = call(
        functools.partial(input_sums_kernel, widths),
        (shape((devices, 1, 128 + 2 * room)),),
        (joined, latent1, row_of(norm3b_g), row_of(norm3b_b)),
        (
            pltpu.VMEM(latent1.shape, bf16),
            pltpu.VMEM((1, shard), f32),
            pltpu.VMEM((1, shard), f32),
            pltpu.SemaphoreType.DMA((4,)),
        ),
        outside=(1, 2, 3),
    )
    sums = exchange(sent)
    near, far, near_edges, far_edges = gathered(joined, received)

    flops_three = 2 * height * whole_cols * 9 * deep * shard
    by_input = lambda weight: jnp.swapaxes(weight, 2, 3)
    tile_out = shape((height, shard, whole_cols), bf16)
    three_scratch = (
        pltpu.VMEM((3 * shard, height * whole_cols), f32),
        pltpu.VMEM((3, 3, shard, deep), bf16),
        pltpu.SemaphoreType.DMA,
    )
    hid3, local, row_three = call(
        functools.partial(level_three_first_kernel, count_three, widths[1], sizes),
        (tile_out, tile_out, shape((1, 128))),
        (near, far, near_edges, far_edges, sums, row_of(norm3a_g), row_of(norm3a_b), by_input(conv3a_w)),
        (pltpu.VMEM((height + 2, whole_cols, deep), bf16), pltpu.VMEM((height, whole_cols, deep), bf16)) + three_scratch,
        flops=flops_three,
        outside=(7,),
    )
    received = [hop_to(hid3, 2 * k) for k in range(1, chips)]
    hid1, sent_two = call(
        functools.partial(level_one_first_kernel, count_one, widths[0], sizes),
        (shape((rows + 3, wide, chans), bf16), shape((devices, 1, 128))),
        (latent1, top, low, beside, sums, row_of(norm1a_g), row_of(norm1a_b), row_three, conv1a_w),
        (
            pltpu.VMEM((rows + 3, wide, 3 * chans), bf16),
            pltpu.VMEM((3 * chans, 3 * chans), bf16),
            pltpu.VMEM(((rows + 3) * wide + 16, 3 * chans), f32),
            pltpu.VMEM((rows + 3, wide, chans), bf16),
            pltpu.SemaphoreType.DMA((2,)),
        ),
        flops=2 * rows * cols * 9 * chans * chans,
        outside_out=(0,),
    )

    sums_two = exchange(sent_two)
    *received, sums_two = lax.optimization_barrier((*received, sums_two))
    near_two, far_two, near_edges_two, far_edges_two = gathered(hid3, received)

    out1 = call(
        functools.partial(level_one_second_kernel, count_one, widths[0], sizes),
        (shape(latent1.shape, bf16),),
        (hid1, latent1, sums_two, row_of(norm1b_g), row_of(norm1b_b), row_of(conv1b_b), conv1b_w),
        (
            pltpu.VMEM((rows + 1, wide, 3 * chans), bf16),
            pltpu.VMEM((3 * chans, 3 * chans), bf16),
            pltpu.VMEM(((rows + 1) * wide + 16, 3 * chans), f32),
        ),
        flops=2 * rows * cols * 9 * chans * chans,
    )
    bias = jnp.pad(row_of(conv3b_b), ((0, 0), (0, room - shard)))
    out3 = call(
        functools.partial(level_three_second_kernel, count_three, widths[1], sizes),
        (tile_out,),
        (near_two, far_two, near_edges_two, far_edges_two, local, sums_two, sums, by_input(conv3b_w), bias),
        (pltpu.VMEM((deep, (height + 2) * whole_cols), bf16),) + three_scratch,
        flops=flops_three,
        outside=(7,),
    )
    return (out1, jnp.swapaxes(out3, 1, 2))


def solution(mesh):
    placed = (
        P("rows", "cols", None),
        P(),
        P(),
        P(),
        P(),
        P(),
        P(),
        P(),
        P("rows", "cols", None),
        P("rows", "cols", None),
        P(),
        P(),
        P(None, None, None, "cols"),
        P("cols"),
        P("cols"),
        P(None, None, None, "cols"),
        P("cols"),
    )
    return jax.shard_map(
        body,
        mesh=mesh,
        in_specs=placed,
        out_specs=(P("rows", "cols", None), P("rows", None, "cols")),
        check_vma=False,
    )
```
